32 devices in a mesh: groups: 2 (over y), seq: 4 (over z), head: 4 (over x, core).
Axes of the slice: x: 2, y: 2, z: 4, core: 2. Of those that a mesh axis runs over, the one named last changes fastest.
Arguments:
- residual: bfloat16 [4096, 2560], P(('groups', 'seq'), 'head'), parts along dimension 0, may hold values from -6 to 6
- x_in: bfloat16 [4096, 5120], P(('groups', 'seq'), 'head'), parts along dimension 0, may hold values from -6 to 6
- bc_in: bfloat16 [4096, 256], P(('groups', 'seq')), parts along dimension 0, may hold values from -1.5 to 1.5
- z_in: bfloat16 [4096, 5120], P(('groups', 'seq'), 'head'), parts along dimension 0, may hold values from -6 to 6
- dt_raw: float32 [80, 4096], P('head', ('groups', 'seq')), parts along dimension 1, may hold values from -5 to 5
- dt_bias: float32 [80], P('head'), may hold values from -3 to 0
- decay_rate: float32 [80], P('head'), may hold values from 0.0003 to 0.15
- d_skip: float32 [80], P('head'), may hold values from 1 to 4
- conv_x_weight: bfloat16 [4, 5120], P(None, 'head'), may hold values from -3 to 3
- conv_x_bias: bfloat16 [5120], P('head'), may hold values from -3 to 3
- conv_bc_weight: bfloat16 [4, 256], replicated, may hold values from -3 to 3
- conv_bc_bias: bfloat16 [256], replicated, may hold values from -3 to 3
- norm_gain: bfloat16 [5120], P('head'), may hold values from 0.5 to 1.5
- out_weight: bfloat16 [5120, 2560], P('head'), may hold values from -0.078125 to 0.078125
- final_gain: bfloat16 [2560], replicated, may hold values from 0.5 to 1.5
- lm_weight: bfloat16 [2560, 25600], P('seq', 'head'), may hold values from -15.811388 to 15.811388
- targets: int32 [4096], P(('groups', 'seq')), parts along dimension 0, may hold values from 0 to 25599
- doc_lengths: int32 [8], P('groups'), parts along dimension 0, may hold values from 1 to 1536, as said below
Outputs:
- block_out: bfloat16 [4096, 2560], P(('groups', 'seq'), 'head'), parts along dimension 0
- doc_loss: float32 [8], P('groups'), parts along dimension 0
The draws below stay inside these ranges and needn't reach their ends.
There are 2 independent parts, one for each index of `groups`. The reference program is written for one: setup_inputs(seed, part) draws one part's arguments, and reference() takes and returns one part's arrays. A program takes and returns all parts, laid end to end along the dimension named above; an argument that names none is the same for every part. Nothing has to cross between parts.
Inputs may be any that keep to these rules, and one draw needn't show every extreme that they name: `doc_lengths`: the lengths of a group's 4 documents, in the order in which they are packed into its 2048 tokens; they sum to 2048.
All inputs are finite; a program needn't handle non-finite values.
Results may differ from the reference program's by a relative error of at most 0.00145.
The reference program's roundings to bfloat16 on the way count: a program that leaves them out, or rounds other values in their place, can miss the bound.
Values may be sent and summed in bfloat16 or wider, within the bound.
A program may use at most 128 MiB of HBM per device.

```python
import math
import jax
import jax.numpy as jnp
import numpy as np
from jax import lax

D = 2560
HEADS = 80
HEAD_SIZE = 64
STATE = 128
KERNEL = 4
VOCAB = 25600
SPAN = 256
TOK_DEV = 512
INNER = 5120
TOKENS = 2048
DOCS = 4
N_SEQ = 4


def draw_lm_weight(key, part):
    entries = jax.random.truncated_normal(jax.random.fold_in(key, 11), -5.0, 5.0, (D, VOCAB), jnp.float32) * (3.0 / math.sqrt(D))
    return entries.astype(jnp.bfloat16)


def draw_doc_lengths(key, part):
    longest = 3 * TOK_DEV
    rest = TOKENS - longest
    others = DOCS - 1
    spacing = rest // others
    jitter = jax.random.randint(jax.random.fold_in(key, 21), (others - 1,), 0, spacing, jnp.int32)
    cuts = (jnp.arange(1, others, dtype=jnp.int32) * spacing + jitter).astype(jnp.int32)
    edges = jnp.concatenate([jnp.zeros((1,), jnp.int32), cuts, jnp.full((1,), rest, jnp.int32)])
    pieces = (edges[1:] - edges[:-1]).astype(jnp.int32)
    joined = jnp.concatenate([pieces, jnp.full((1,), longest, jnp.int32)])
    place = jax.random.randint(jax.random.fold_in(key, 22), (), 0, DOCS, jnp.int32)
    order = jnp.arange(DOCS, dtype=jnp.int32)
    index = jnp.where(order < place, order, jnp.where(order == place, others, order - 1)).astype(jnp.int32)
    return joined[index]


def plant(array, own_key, least, largest):
    longest = array.shape.index(max(array.shape))
    spots = []
    for shift in (0, 1):
        where = [jax.random.randint(jax.random.fold_in(own_key, axis), (), 0, length) for axis, length in enumerate(array.shape)]
        where[longest] = (where[longest] + shift) % array.shape[longest]
        spots.append(tuple(where))
    return array.at[spots[0]].set(least).at[spots[1]].set(largest)


def steps_of(own_key, shape, split, low, high):
    gain = 1.0
    for axis_at, blocks in split:
        draws = jax.random.uniform(jax.random.fold_in(jax.random.fold_in(own_key, 6), axis_at), (blocks,), jnp.float32, low / len(split), high / len(split))
        gain = gain * jnp.repeat(jnp.exp(draws), shape[axis_at] // blocks).reshape((-1,) + (1,) * (len(shape) - 1 - axis_at))
    return gain


def rank_bounds(amount, lean):
    portions = [(1 << 20) // math.isqrt(standing ** lean) + 1 for standing in range(1, amount + 1)]
    width = 1 + sum(portions) // (1 << 30)
    return np.cumsum(np.array([max(1, weight // width) for weight in portions]))


def skewed_ids(rng, shape, number_of, slope):
    listing = rank_bounds(number_of, slope)
    lot = jax.random.randint(jax.random.fold_in(rng, 1), shape, 0, int(listing[number_of - 1]))
    rank = jnp.searchsorted(jnp.asarray(listing, jnp.int32), lot, side="right")
    return jax.random.permutation(jax.random.fold_in(rng, 2), number_of)[rank].astype(jnp.int32)


def gaussian(rng, dims, width, limit, shards=(), kind=jnp.bfloat16):
    result = jax.random.normal(rng, dims, jnp.float32) * width
    if len(shards) > 0:
        result = steps_of(rng, dims, shards, -0.22, 0.18) * result
    return jnp.clip(result, min=-limit, max=limit).astype(kind)


def setup_inputs(seed: int = 0, part: int = 0) -> dict:
    arg_keys = jax.random.split(jax.random.key(seed), 19)
    part_splits = jax.random.split(jax.random.fold_in(arg_keys[18], part), 19)
    return {
        "residual": gaussian(part_splits[0], (TOKENS, D), 1.0, 6.0, ((0, 4), (1, 4))),
        "x_in": gaussian(part_splits[1], (TOKENS, INNER), 1.0, 6.0, ((0, 4), (1, 4))),
        "bc_in": gaussian(part_splits[2], (TOKENS, 2 * STATE), 0.25, 1.5, ((0, 4),)),
        "z_in": gaussian(part_splits[3], (TOKENS, INNER), 1.0, 6.0, ((0, 4), (1, 4))),
        "dt_raw": gaussian(part_splits[4], (HEADS, TOKENS), 1.0, 5.0, ((0, 4), (1, 4)), jnp.float32),
        "dt_bias": jnp.clip(-3.0 + 3.0 * jax.random.uniform(arg_keys[5], (HEADS,), jnp.float32) ** steps_of(arg_keys[5], (HEADS,), ((0, 4),), -0.2, 0.2), -3.0, 0.0),
        "decay_rate": jnp.clip(jnp.exp(math.log(0.15) - 6.214608 * jax.random.uniform(arg_keys[6], (HEADS,), jnp.float32) ** steps_of(arg_keys[6], (HEADS,), ((0, 4),), -0.2, 0.2)), 0.0003, 0.15),
        "d_skip": jnp.clip(1.0 + 3.0 * jax.random.uniform(arg_keys[7], (HEADS,), jnp.float32) ** steps_of(arg_keys[7], (HEADS,), ((0, 4),), -0.2, 0.2), 1.0, 4.0),
        "conv_x_weight": gaussian(arg_keys[8], (KERNEL, INNER), KERNEL ** -0.5, 3.0, ((1, 4),)),
        "conv_x_bias": gaussian(arg_keys[9], (INNER,), 0.5, 3.0, ((0, 4),)),
        "conv_bc_weight": gaussian(arg_keys[10], (KERNEL, 2 * STATE), KERNEL ** -0.5, 3.0),
        "conv_bc_bias": gaussian(arg_keys[11], (2 * STATE,), 0.5, 3.0),
        "norm_gain": jnp.clip(1.0 + 0.1 * jax.random.normal(arg_keys[12], (INNER,), jnp.float32), 0.5, 1.5).astype(jnp.bfloat16),
        "out_weight": gaussian(arg_keys[13], (INNER, D), INNER ** -0.5, 0.078125, ((0, 4),)),
        "final_gain": jnp.clip(1.0 + 0.1 * jax.random.normal(arg_keys[14], (D,), jnp.float32), 0.5, 1.5).astype(jnp.bfloat16),
        "lm_weight": draw_lm_weight(jax.random.fold_in(arg_keys[18], 71), part),
        "targets": plant(skewed_ids(part_splits[16], (TOKENS,), VOCAB, 2), jax.random.fold_in(part_splits[16], 3), 0, VOCAB - 1).astype(jnp.int32),
        "doc_lengths": draw_doc_lengths(jax.random.fold_in(jax.random.fold_in(arg_keys[18], part), 71), part),
    }


EPSILON = 1e-05
HIGH = lax.Precision.HIGHEST

def document_of(positions, doc_lengths):
    starts = jnp.cumsum(doc_lengths) - doc_lengths
    return lax.optimization_barrier(jnp.sum((positions[:, None] >= starts[None, :]).astype(jnp.int32), axis=1)) - 1

def causal_conv(signal, rim_rows, weight, bias, positions, doc_ids, doc_lengths):
    length = signal.shape[0]
    taps = weight.shape[0]
    joined = jnp.concatenate([rim_rows, signal], axis=0).astype(jnp.float32)
    total = jnp.zeros(signal.shape, jnp.float32) + bias.astype(jnp.float32)[None, :]
    for offset in range(taps):
        lag = taps - 1 - offset
        source = document_of(positions - lag, doc_lengths)
        same = (source == doc_ids).astype(jnp.float32)
        total = total + weight[offset].astype(jnp.float32)[None, :] * joined[offset:offset + length] * same[:, None]
    return jax.nn.silu(total).astype(jnp.bfloat16)

def span_step(state, pieces, rates):
    signal, bmat, cmat, steps, doc_ids, doc_prev = pieces
    signal = signal.astype(jnp.float32)
    bmat = bmat.astype(jnp.float32)
    cmat = cmat.astype(jnp.float32)
    climb = jnp.cumsum(steps * rates[:, None], axis=1)
    extent = doc_ids.shape[0]
    order = jnp.arange(extent, dtype=jnp.int32)
    inside = (doc_ids[:, None] == doc_ids[None, :]) & (order[:, None] >= order[None, :])
    gap = climb[:, :, None] - climb[:, None, :]
    decay = jnp.where(inside[None], jnp.exp(-jnp.where(inside[None], gap, 0.0)), 0.0)
    scores = jnp.dot(cmat, bmat.T, precision=HIGH)
    weights = decay * scores[None] * steps[:, None, :]
    output = jnp.einsum('hts,shp->thp', weights, signal, precision=HIGH)
    carried = (doc_ids == doc_prev).astype(jnp.float32)
    entry = jnp.exp(-climb) * carried[None, :]
    output = output + jnp.einsum('tn,hpn->thp', cmat, state, precision=HIGH) * entry.T[:, :, None]
    last = doc_ids[extent - 1]
    tail = jnp.exp(climb - climb[:, extent - 1:]) * (doc_ids == last).astype(jnp.float32)[None, :] * steps
    kept = jnp.exp(-climb[:, extent - 1]) * (last == doc_prev).astype(jnp.float32)
    fresh = jnp.einsum('hs,shp,sn->hpn', tail, signal, bmat, precision=HIGH)
    return (kept[:, None, None] * state + fresh, output)

def reference(residual, x_in, bc_in, z_in, dt_raw, dt_bias, decay_rate, d_skip, conv_x_weight, conv_x_bias, conv_bc_weight, conv_bc_bias, norm_gain, out_weight, final_gain, lm_weight, targets, doc_lengths):
    positions = jnp.arange(TOKENS, dtype=jnp.int32)
    doc_ids = document_of(positions, doc_lengths)
    margin = KERNEL - 1
    signal = causal_conv(x_in, jnp.zeros((margin, INNER), jnp.bfloat16), conv_x_weight, conv_x_bias, positions, doc_ids, doc_lengths)
    keys_queries = causal_conv(bc_in, jnp.zeros((margin, 2 * STATE), jnp.bfloat16), conv_bc_weight, conv_bc_bias, positions, doc_ids, doc_lengths)
    steps = jax.nn.softplus(dt_raw + dt_bias[:, None])
    blocks = TOKENS // SPAN
    block_starts = jnp.arange(blocks, dtype=jnp.int32) * SPAN
    pieces = (signal.reshape(blocks, SPAN, HEADS, HEAD_SIZE), keys_queries[:, :STATE].reshape(blocks, SPAN, STATE), keys_queries[:, STATE:].reshape(blocks, SPAN, STATE), steps.reshape(HEADS, blocks, SPAN).transpose(1, 0, 2), doc_ids.reshape(blocks, SPAN), document_of(block_starts - 1, doc_lengths))

    def advance(state, piece):
        return span_step(state, piece, decay_rate)
    ignored, outputs = lax.scan(advance, jnp.zeros((HEADS, HEAD_SIZE, STATE), jnp.float32), pieces)
    mixed = outputs.reshape(TOKENS, HEADS, HEAD_SIZE) + d_skip[None, :, None] * signal.reshape(TOKENS, HEADS, HEAD_SIZE).astype(jnp.float32)
    gated = mixed.reshape(TOKENS, INNER) * jax.nn.silu(z_in.astype(jnp.float32))
    scale = lax.rsqrt(lax.optimization_barrier(jnp.sum(gated * gated, axis=1)) / INNER + EPSILON)
    normed = (gated * scale[:, None] * norm_gain.astype(jnp.float32)[None, :]).astype(jnp.bfloat16)
    projected = jnp.dot(normed, out_weight, preferred_element_type=jnp.float32)
    block_out = (residual.astype(jnp.float32) + projected).astype(jnp.bfloat16)
    widened = block_out.astype(jnp.float32)
    final_scale = lax.rsqrt(lax.optimization_barrier(jnp.sum(widened * widened, axis=1)) / D + EPSILON)
    hidden = (widened * final_scale[:, None] * final_gain.astype(jnp.float32)[None, :]).astype(jnp.bfloat16)

    def token_loss(piece):
        hidden_rows, target_rows = piece
        logits = jnp.dot(hidden_rows, lm_weight, preferred_element_type=jnp.float32)
        peak = lax.optimization_barrier(jnp.max(logits, axis=1))
        total = lax.optimization_barrier(jnp.sum(jnp.exp(logits - peak[:, None]), axis=1))
        column = jnp.arange(VOCAB, dtype=jnp.int32)
        picked = lax.optimization_barrier(jnp.sum(jnp.where(column[None, :] == target_rows[:, None], logits, 0.0), axis=1))
        return peak + jnp.log(total) - picked
    losses = lax.map(token_loss, (hidden.reshape(N_SEQ, TOK_DEV, D), targets.reshape(N_SEQ, TOK_DEV))).reshape(TOKENS)
    member = (doc_ids[:, None] == jnp.arange(DOCS, dtype=jnp.int32)[None, :]).astype(jnp.float32)
    sums = jnp.dot(losses, member, precision=HIGH)
    return (block_out, sums / doc_lengths.astype(jnp.float32))
```

```python
import jax
import jax.numpy as jnp
from jax import lax
from jax.experimental import pallas as pl
from jax.experimental.pallas import tpu as pltpu
from jax.sharding import PartitionSpec as P

D = 2560
HEAD_SIZE = 64
STATE = 128
KERNEL = 4
SPAN = 256
INNER = 5120


EPSILON = 1e-05
HIGH = lax.Precision.HIGHEST
HALF = lax.Precision.HIGH
LOW = -1e30


def shifted(array, axis, by):
    length = lax.axis_size(axis)
    pairs = [(i, i + by) for i in range(length) if 0 <= i + by < length]
    return lax.ppermute(array, axis, pairs)


def rotated(array, axis, by):
    length = lax.axis_size(axis)
    return lax.ppermute(array, axis, [(i, (i + by) % length) for i in range(length)])


def sibling(array, axis):
    length = lax.axis_size(axis)
    return lax.ppermute(array, axis, [(i, i ^ 1) for i in range(length)])


def scattered_product(normed, weight, axis):
    length = lax.axis_size(axis)
    rank = lax.axis_index(axis)
    chips = length // 2
    share = weight.shape[1] // length

    def columns(core):
        return jnp.concatenate(
            [
                lax.dynamic_slice_in_dim(
                    weight, ((rank // 2 + by) % chips * 2 + core) * share, share, 1
                )
                for by in range(chips)
            ],
            axis=1,
        )

    theirs = columns(1 - rank % 2)
    ours = columns(rank % 2)
    other = jnp.dot(normed, theirs, preferred_element_type=jnp.float32)
    arrived = sibling(other, axis)
    pair = jnp.dot(normed, ours, preferred_element_type=jnp.float32) + arrived
    total = pair[:, :share]
    for by in range(1, chips):
        total = total + rotated(pair[:, by * share : (by + 1) * share], axis, 2 * by)
    return total


def gathered_features(part, axis):
    length = lax.axis_size(axis)
    rank = lax.axis_index(axis)
    chips = length // 2
    rows, share = part.shape
    column = [part] + [rotated(part, axis, 2 * by) for by in range(1, chips)]
    joined = jnp.concatenate(column, axis=1)
    twin = sibling(joined, axis)
    full = jnp.zeros((rows, share * length), part.dtype)
    for by in range(chips):
        source = (rank + 2 * (chips - by)) % length
        piece = slice(by * share, (by + 1) * share)
        full = lax.dynamic_update_slice_in_dim(full, joined[:, piece], source * share, 1)
        full = lax.dynamic_update_slice_in_dim(full, twin[:, piece], (source ^ 1) * share, 1)
    return full


def entering(through, state, axis):
    length = lax.axis_size(axis)
    tag = jnp.broadcast_to(through[:, None, None], (through.shape[0], 8, state.shape[2]))
    packed = shifted(jnp.concatenate([state, tag], axis=1), axis, 1)
    extent = state.shape[1]
    reach = 1
    while reach < length:
        earlier = shifted(packed, axis, reach)
        decay = packed[:, extent : extent + 1, :]
        packed = jnp.concatenate(
            [packed[:, :extent] + decay * earlier[:, :extent], decay * earlier[:, extent:]], axis=1
        )
        reach *= 2
    return packed[:, :extent]


def document_of(positions, doc_lengths):
    starts = jnp.cumsum(doc_lengths) - doc_lengths
    return jnp.sum((positions[:, None] >= starts[None, :]).astype(jnp.int32), axis=1) - 1


def causal_conv(signal, rim_rows, weight, bias, positions, doc_ids, doc_lengths):
    length = signal.shape[0]
    taps = weight.shape[0]
    joined = jnp.concatenate([rim_rows, signal], axis=0).astype(jnp.float32)
    total = jnp.zeros(signal.shape, jnp.float32) + bias.astype(jnp.float32)[None, :]
    for offset in range(taps):
        lag = taps - 1 - offset
        source = document_of(positions - lag, doc_lengths)
        same = (source == doc_ids).astype(jnp.float32)
        total = (
            total
            + weight[offset].astype(jnp.float32)[None, :]
            * joined[offset : offset + length]
            * same[:, None]
        )
    return jax.nn.silu(total).astype(jnp.bfloat16)


def conv_state_kernel(x_ref, rim_ref, taps_ref, bias_ref, same_ref, cols_ref, bmat_ref, values_ref, state_ref, held):
    length, lanes = x_ref.shape
    taps = taps_ref.shape[0]
    held[0:8, :] = rim_ref[...].astype(jnp.float32)
    held[8:, :] = x_ref[...].astype(jnp.float32)
    total = jnp.zeros((length, lanes), jnp.float32) + bias_ref[...]
    for offset in range(taps):
        lag = taps - 1 - offset
        rows = held[8 - lag : 8 - lag + length, :]
        total = total + taps_ref[offset : offset + 1, :] * rows * same_ref[:, lag : lag + 1]
    values = jax.nn.silu(total).astype(jnp.bfloat16)
    values_ref[...] = values
    first = lax.broadcasted_iota(jnp.int32, (length, lanes), 1) < HEAD_SIZE
    tail = jnp.where(first, cols_ref[0, :, 2:3], cols_ref[0, :, 3:4])
    scaled = values.astype(jnp.float32) * tail
    high = scaled.astype(jnp.bfloat16)
    low = (scaled - high.astype(jnp.float32)).astype(jnp.bfloat16)
    bmat = bmat_ref[...]
    dims = (((0,), (0,)), ((), ()))
    state_ref[...] = lax.dot_general(
        high, bmat, dims, preferred_element_type=jnp.float32
    ) + lax.dot_general(low, bmat, dims, preferred_element_type=jnp.float32)


def within_kernel(values_ref, scores_ref, cols_ref, rows_ref, skip_ref, out_ref):
    length, lanes = values_ref.shape
    for cut in range(0, length, SPAN):
        upto = cut + SPAN
        values = values_ref[0:upto, :]
        scores = scores_ref[cut:upto, 0:upto]
        parts = []
        for which in range(2):
            gap = rows_ref[0, which : which + 1, 0:upto] - cols_ref[0, cut:upto, which : which + 1]
            weights = (
                jnp.exp(jnp.minimum(gap, 0.0)) * scores * rows_ref[0, 2 + which : 3 + which, 0:upto]
            )
            high = weights.astype(jnp.bfloat16)
            low = (weights - high.astype(jnp.float32)).astype(jnp.bfloat16)
            parts.append(
                jnp.dot(high, values, preferred_element_type=jnp.float32)
                + jnp.dot(low, values, preferred_element_type=jnp.float32)
            )
        first = lax.broadcasted_iota(jnp.int32, (SPAN, lanes), 1) < HEAD_SIZE
        own = values_ref[cut:upto, :].astype(jnp.float32)
        out_ref[cut:upto, :] = jnp.where(first, parts[0], parts[1]) + skip_ref[...] * own


def conv_state(x_in, rim, taps, bias, same, cols, bmat):
    length, inner_here = x_in.shape
    lanes = 2 * HEAD_SIZE
    return pl.pallas_call(
        conv_state_kernel,
        grid=(inner_here // lanes,),
        in_specs=[
            pl.BlockSpec((length, lanes), lambda i: (0, i)),
            pl.BlockSpec((8, lanes), lambda i: (0, i)),
            pl.BlockSpec((taps.shape[0], lanes), lambda i: (0, i)),
            pl.BlockSpec((1, lanes), lambda i: (0, i)),
            pl.BlockSpec(same.shape, lambda i: (0, 0)),
            pl.BlockSpec((1, length, 4), lambda i: (i, 0, 0)),
            pl.BlockSpec(bmat.shape, lambda i: (0, 0)),
        ],
        out_specs=[
            pl.BlockSpec((length, lanes), lambda i: (0, i)),
            pl.BlockSpec((lanes, STATE), lambda i: (i, 0)),
        ],
        out_shape=[
            jax.ShapeDtypeStruct((length, inner_here), jnp.bfloat16),
            jax.ShapeDtypeStruct((inner_here, STATE), jnp.float32),
        ],
        scratch_shapes=[pltpu.VMEM((length + 8, lanes), jnp.float32)],
        cost_estimate=pl.CostEstimate(flops=10**9, bytes_accessed=6 * 10**6, transcendentals=10**6),
    )(x_in, rim, taps, bias, same, cols, bmat)


def within(values, scores, cols, rows, skip):
    length, inner_here = values.shape
    lanes = 2 * HEAD_SIZE
    return pl.pallas_call(
        within_kernel,
        grid=(inner_here // lanes,),
        in_specs=[
            pl.BlockSpec((length, lanes), lambda i: (0, i)),
            pl.BlockSpec(scores.shape, lambda i: (0, 0)),
            pl.BlockSpec((1, length, 4), lambda i: (i, 0, 0)),
            pl.BlockSpec((1, 4, length), lambda i: (i, 0, 0)),
            pl.BlockSpec((1, lanes), lambda i: (0, i)),
        ],
        out_specs=pl.BlockSpec((length, lanes), lambda i: (0, i)),
        out_shape=jax.ShapeDtypeStruct((length, inner_here), jnp.float32),
        cost_estimate=pl.CostEstimate(flops=8 * 10**9, bytes_accessed=20 * 10**6, transcendentals=10**7),
    )(values, scores, cols, rows, skip)


def local(
    residual,
    x_in,
    bc_in,
    z_in,
    dt_raw,
    dt_bias,
    decay_rate,
    d_skip,
    conv_x_weight,
    conv_x_bias,
    conv_bc_weight,
    conv_bc_bias,
    norm_gain,
    out_weight,
    final_gain,
    lm_weight,
    targets,
    doc_lengths,
):
    length = x_in.shape[0]
    inner_here = x_in.shape[1]
    heads_here = dt_raw.shape[0]
    seq_rank = lax.axis_index("seq")
    head_rank = lax.axis_index("head")
    offset_here = seq_rank * length
    positions = offset_here + jnp.arange(length, dtype=jnp.int32)
    doc_ids = document_of(positions, doc_lengths)
    columns_here = lm_weight.shape[1]
    devices = lax.axis_size("seq")
    width = -(-columns_here // (devices * 128)) * 128

    def window(rank):
        return jnp.minimum(rank * width, columns_here - width)

    depth = lm_weight.shape[0]
    vocab_weight = jnp.zeros((depth * devices, width), lm_weight.dtype)
    group = lax.axis_index("groups")
    groups = lax.axis_size("groups")
    band = depth // groups
    pieces = [
        lax.dynamic_slice(
            lm_weight, (group * band, window((seq_rank + by) % devices)), (band, width)
        )
        for by in range(1, devices)
    ]
    aims = [targets]
    for by in range(1, devices):
        aims.append(rotated(targets, "seq", by))
    margin = KERNEL - 1
    rims = shifted(
        jnp.concatenate([x_in[length - margin :], bc_in[length - margin :]], axis=1), "seq", 1
    )
    x_rim, bc_rim = rims[:, :inner_here], rims[:, inner_here:]
    keys_queries = causal_conv(
        bc_in, bc_rim, conv_bc_weight, conv_bc_bias, positions, doc_ids, doc_lengths
    )
    bmat, cmat = keys_queries[:, :STATE], keys_queries[:, STATE:]
    steps = jax.nn.softplus(dt_raw + dt_bias[:, None])
    climb = jnp.cumsum(steps * decay_rate[:, None], axis=1)
    before = document_of(jnp.reshape(offset_here - 1, (1,)), doc_lengths)[0]
    carried = (doc_ids == before).astype(jnp.float32)
    through = jnp.exp(-climb[:, length - 1]) * carried[length - 1]
    same = jnp.stack(
        [
            (document_of(positions - lag, doc_lengths) == doc_ids).astype(jnp.float32)
            for lag in range(KERNEL)
        ],
        axis=1,
    )
    last = (doc_ids == doc_ids[length - 1]).astype(jnp.float32)
    tail = jnp.exp(climb - climb[:, length - 1 :]) * last[None, :] * steps
    couples = heads_here // 2
    rows = jnp.concatenate(
        [climb.reshape(couples, 2, length), steps.reshape(couples, 2, length)], axis=1
    )
    cols = jnp.concatenate(
        [climb.reshape(couples, 2, length), tail.reshape(couples, 2, length)], axis=1
    ).transpose(0, 2, 1)
    rim = jnp.concatenate([jnp.zeros((8 - margin, inner_here), x_rim.dtype), x_rim], axis=0)
    values, own_end = conv_state(
        x_in,
        rim,
        conv_x_weight.astype(jnp.float32),
        conv_x_bias.astype(jnp.float32)[None, :],
        same,
        cols,
        bmat,
    )
    of_head = jnp.arange(inner_here, dtype=jnp.int32)[None, :] // HEAD_SIZE
    spread = (of_head == jnp.arange(heads_here, dtype=jnp.int32)[:, None]).astype(jnp.float32)
    incoming = entering(
        through, own_end.reshape(heads_here, HEAD_SIZE, STATE), "seq"
    ).reshape(inner_here, STATE)
    held_back = lax.optimization_barrier(tuple(pieces[1:]) + (incoming,))
    pieces, incoming = pieces[:1] + list(held_back[:-1]), held_back[-1]
    arrivals = []
    for by in range(1, devices):
        arrivals.append(rotated(pieces[by - 1], "seq", by))
    bands = []
    for by in range(1, devices):
        bands.append(
            [arrivals[by - 1]]
            + [rotated(arrivals[by - 1], "groups", hop) for hop in range(1, groups)]
        )
    order = jnp.arange(length, dtype=jnp.int32)
    inside = (doc_ids[:, None] == doc_ids[None, :]) & (order[:, None] >= order[None, :])
    scores = jnp.where(
        inside,
        lax.dot_general(
            cmat, bmat, (((1,), (1,)), ((), ())), preferred_element_type=jnp.float32
        ),
        0.0,
    )
    skip = jnp.dot(d_skip[None, :], spread, precision=HIGH)
    output = within(values, scores, cols, rows, skip)
    entry = jnp.dot((jnp.exp(-climb) * carried[None, :]).T, spread, precision=HIGH)
    arriving = lax.dot_general(
        cmat.astype(jnp.float32), incoming, (((1,), (1,)), ((), ())), precision=HALF
    )
    gated = (output + arriving * entry) * jax.nn.silu(z_in.astype(jnp.float32))
    square_sum = lax.psum(jnp.sum(gated * gated, axis=1), "head")
    scale = lax.rsqrt(square_sum / INNER + EPSILON)
    normed = (gated * scale[:, None] * norm_gain.astype(jnp.float32)[None, :]).astype(jnp.bfloat16)
    share = residual.shape[1]
    projected = scattered_product(normed, out_weight, "head")
    block_out = (residual.astype(jnp.float32) + projected).astype(jnp.bfloat16)
    widened = block_out.astype(jnp.float32)
    square_total = lax.psum(jnp.sum(widened * widened, axis=1), "head")
    gain_part = lax.dynamic_slice_in_dim(final_gain, head_rank * share, share, 0)
    final_scale = lax.rsqrt(square_total / D + EPSILON)
    hidden_part = (widened * final_scale[:, None] * gain_part.astype(jnp.float32)[None, :]).astype(
        jnp.bfloat16
    )
    own = lax.dynamic_slice_in_dim(lm_weight, window(seq_rank), width, 1)
    vocab_weight = lax.dynamic_update_slice_in_dim(vocab_weight, own, seq_rank * depth, 0)
    for by in range(1, devices):
        source = (seq_rank + devices - by) % devices
        for hop in range(groups):
            start = source * depth + (group + groups - hop) % groups * band
            vocab_weight = lax.dynamic_update_slice_in_dim(
                vocab_weight, bands[by - 1][hop], start, 0
            )
    column = jnp.arange(width, dtype=jnp.int32)
    first = head_rank * columns_here + window(seq_rank)
    live = column + window(seq_rank) >= seq_rank * width
    marks = jnp.zeros((3, length * devices), jnp.float32)
    for by in range(devices):
        source = (seq_rank + devices - by) % devices
        if by and by % 4 == 0:
            hidden_part, marks = lax.optimization_barrier((hidden_part, marks))
        rows = rotated(hidden_part, "seq", by) if by else hidden_part
        hidden = gathered_features(rows, "head")
        logits = jnp.dot(hidden, vocab_weight, preferred_element_type=jnp.float32)
        logits = jnp.where(live[None, :], logits, LOW)
        peak = jnp.max(logits, axis=1)
        wanted = aims[by] - first
        total = jnp.sum(jnp.exp(logits - peak[:, None]), axis=1)
        picked = jnp.sum(
            jnp.where((column[None, :] == wanted[:, None]) & live[None, :], logits, 0.0), axis=1
        )
        marks = lax.dynamic_update_slice_in_dim(
            marks, jnp.stack([peak, total, picked]), source * length, 1
        )
    for axis in ("head", "seq"):
        every_mark = lax.all_gather(marks, axis)
        peak = jnp.max(every_mark[:, 0], axis=0)
        total = jnp.sum(every_mark[:, 1] * jnp.exp(every_mark[:, 0] - peak[None]), axis=0)
        marks = jnp.stack([peak, total, jnp.sum(every_mark[:, 2], axis=0)])
    losses = marks[0] + jnp.log(marks[1]) - marks[2]
    every = document_of(jnp.arange(length * devices, dtype=jnp.int32), doc_lengths)
    documents = jnp.arange(doc_lengths.shape[0], dtype=jnp.int32)
    member = every[None, :] == documents[:, None]
    sums = jnp.sum(jnp.where(member, losses[None, :], 0.0), axis=1)
    return (block_out, sums / doc_lengths.astype(jnp.float32))


def solution(mesh):
    in_specs = (
        P(("groups", "seq"), "head"),
        P(("groups", "seq"), "head"),
        P(("groups", "seq"), None),
        P(("groups", "seq"), "head"),
        P("head", ("groups", "seq")),
        P("head"),
        P("head"),
        P("head"),
        P(None, "head"),
        P("head"),
        P(),
        P(),
        P("head"),
        P("head", None),
        P(),
        P("seq", "head"),
        P(("groups", "seq")),
        P("groups"),
    )
    out_specs = (P(("groups", "seq"), "head"), P("groups"))


    return jax.shard_map(local, mesh=mesh, in_specs=in_specs, out_specs=out_specs, check_vma=False)
```
